32 devices in a mesh: seq: 8 (over z, x), mp: 4 (over y, core).
Axes of the slice: x: 2, y: 2, z: 4, core: 2. Of those that a mesh axis runs over, the one named last changes fastest.
Arguments:
- branch_in: bfloat16 [4096, 4096], P('seq', 'mp'), may hold values from -48 to 48
- branch_gate: bfloat16 [4096, 4096], P('seq', 'mp'), may hold values from -6 to 6
- conv_taps: float32 [4, 4096], P(None, 'mp'), may hold values from -3 to 3
- conv_shift: float32 [4096], P('mp'), may hold values from -3 to 3
- inflow_weight: bfloat16 [16, 256, 256], P('mp'), may hold values from -0.375 to 0.375
- inflow_bias: float32 [4096], P('mp'), may hold values from -4 to 4
- decay_weight: bfloat16 [16, 256, 256], P('mp'), may hold values from -0.375 to 0.375
- decay_bias: float32 [4096], P('mp'), may hold values from -12 to -1.5
- decay_param: float32 [4096], P('mp'), may hold values from 3 to 4
- stream: bfloat16 [4096, 4096], P('seq', 'mp'), may hold values from -48 to 48
- norm_gain: float32 [4096], P('mp'), may hold values from 0.5 to 1.5
- memory_weight: bfloat16 [4096, 512], P('mp'), may hold values from -1 to 1
- queries: bfloat16 [4096, 4096], P('seq', 'mp'), may hold values from -128 to 128
Outputs:
- recurrent_out: bfloat16 [4096, 4096], P('seq', 'mp')
- attended: bfloat16 [4096, 4096], P('seq', 'mp')
The draws below stay inside these ranges and needn't reach their ends.
All inputs are finite; a program needn't handle non-finite values.
Results may differ from the reference program's by a relative error of at most 0.0071.
Values may be sent and summed in bfloat16 or wider, within the bound.
A program may use at most 128 MiB of HBM per device.

```python
import jax
import jax.numpy as jnp
from jax import lax

D = 4096
R = 4096
H = 16
HD = 256
RHEADS = 16
CONV = 4
WINDOW = 2048
TOK_DEV = 512
BLK = 256
TOTAL_TOKENS = 4096


def stream_values(key):
    combined_result = jax.random.fold_in(key, 101)
    noise = jax.random.normal(jax.random.fold_in(combined_result, 1), (TOTAL_TOKENS, D), jnp.float32)
    row_scale = jnp.exp(jax.random.uniform(jax.random.fold_in(combined_result, 2), (TOTAL_TOKENS, 1), jnp.float32, jnp.log(0.25), jnp.log(2.5)))
    column_incline = jnp.exp(jnp.linspace(jnp.log(0.6), jnp.log(1.8), D))
    values = noise * column_incline[None, :] * row_scale
    return jnp.clip(values, -48.0, 48.0)


def gain_values(key):
    return jax.random.uniform(jax.random.fold_in(key, 201), (D,), jnp.float32, 0.5, 1.5)


def memory_values(key):
    return jax.random.normal(jax.random.fold_in(key, 301), (D, 2 * HD), jnp.float32) * D ** (-0.5)


def draw_stream(key, part):
    return stream_values(key).astype(jnp.bfloat16)


def draw_norm_gain(key, part):
    return gain_values(key)


def draw_memory_weight(key, part):
    return jnp.clip(memory_values(key), -1.0, 1.0).astype(jnp.bfloat16)


def draw_queries(key, part):
    combined_result = jax.random.fold_in(key, 401)
    values = jax.random.normal(jax.random.fold_in(combined_result, 1), (TOTAL_TOKENS, H * HD), jnp.float32)
    return jnp.clip(values, -128.0, 128.0).astype(jnp.bfloat16)


def draw_branch_in(key, part):
    combined_result = jax.random.fold_in(key, 501)
    values = jax.random.normal(jax.random.fold_in(combined_result, 1), (TOTAL_TOKENS, R), jnp.float32)
    spike_locations = jax.random.randint(jax.random.fold_in(combined_result, 2), (8,), 0, TOTAL_TOKENS)
    raised_values = jnp.zeros((TOTAL_TOKENS,), jnp.float32).at[spike_locations].set(7.0)
    return jnp.clip(values * (1.0 + raised_values)[:, None], -48.0, 48.0).astype(jnp.bfloat16)


def draw_decay_param(key, part):
    rates = jnp.exp(jax.random.uniform(jax.random.fold_in(key, 601), (R,), jnp.float32, jnp.log(0.02), jnp.log(0.04)))
    return -jnp.log(jnp.expm1(rates))


def draw_decay_bias(key, part):
    combined_result = jax.random.fold_in(key, 701)
    quick_share = 0.5
    quick_mask = jax.random.uniform(jax.random.fold_in(combined_result, 1), (R,), jnp.float32) < quick_share
    quick_bias = jax.random.uniform(jax.random.fold_in(combined_result, 2), (R,), jnp.float32, -2.5, -1.8)
    slow_bias = jax.random.uniform(jax.random.fold_in(combined_result, 3), (R,), jnp.float32, -1.3, 0.0) - jnp.log(1.0 * TOK_DEV)
    return jnp.where(quick_mask, quick_bias, slow_bias)


def block_scale(rng, extent, shards, smallest, largest):
    level = 1.0
    for dim, blocks in shards:
        heights = jax.random.uniform(jax.random.fold_in(jax.random.fold_in(rng, 6), dim), (blocks,), jnp.float32, smallest / len(shards), largest / len(shards))
        level = level * jnp.repeat(jnp.exp(heights), extent[dim] // blocks).reshape((-1,) + (1,) * (len(extent) - 1 - dim))
    return level


def centred(rng, extent, spread, reach, split=(), held_as=jnp.bfloat16):
    loudness = block_scale(rng, extent, split, -0.22, 0.18) if split else 1.0
    result = jax.random.normal(rng, extent, jnp.float32) * spread * loudness
    return jnp.minimum(jnp.maximum(result, -reach), reach).astype(held_as)


def setup_inputs(seed: int = 0) -> dict:
    key_list = jax.random.split(jax.random.key(seed), 14)
    branch_in = draw_branch_in(jax.random.fold_in(key_list[13], 71), 0)
    branch_gate = centred(key_list[1], (TOTAL_TOKENS, R), 1.0, 6.0, ((0, 8), (1, 4)))
    conv_taps = centred(key_list[2], (CONV, R), CONV ** -0.5, 3.0, ((1, 4),), jnp.float32)
    conv_shift = centred(key_list[3], (R,), 0.5, 3.0, ((0, 4),), jnp.float32)
    inflow_weight = centred(key_list[4], (RHEADS, BLK, BLK), BLK ** -0.5, 0.375, ((0, 4),))
    inflow_bias = centred(key_list[5], (R,), 1.0, 4.0, ((0, 4),), jnp.float32)
    decay_weight = centred(key_list[6], (RHEADS, BLK, BLK), BLK ** -0.5, 0.375, ((0, 4),))
    decay_bias = draw_decay_bias(jax.random.fold_in(key_list[13], 71), 0)
    decay_param = draw_decay_param(jax.random.fold_in(key_list[13], 71), 0)
    stream = draw_stream(jax.random.fold_in(key_list[13], 71), 0)
    norm_gain = draw_norm_gain(jax.random.fold_in(key_list[13], 71), 0)
    memory_weight = draw_memory_weight(jax.random.fold_in(key_list[13], 71), 0)
    queries = draw_queries(jax.random.fold_in(key_list[13], 71), 0)
    return dict(branch_in=branch_in, branch_gate=branch_gate, conv_taps=conv_taps, conv_shift=conv_shift, inflow_weight=inflow_weight, inflow_bias=inflow_bias, decay_weight=decay_weight, decay_bias=decay_bias, decay_param=decay_param, stream=stream, norm_gain=norm_gain, memory_weight=memory_weight, queries=queries)


decay_power = 8.0
norm_epsilon = 1e-06
masked_score = -1e+30

def convolve(branch_in, conv_taps, conv_shift):
    inputs = branch_in.astype(jnp.float32)
    totals = conv_shift[None, :] + conv_taps[0][None, :] * inputs
    for offset in range(1, CONV):
        delayed = jnp.concatenate([jnp.zeros((offset, inputs.shape[1]), jnp.float32), inputs[:-offset]], axis=0)
        totals = totals + conv_taps[offset][None, :] * delayed
    return totals.astype(jnp.bfloat16)

def attend_block(query_block, window_block, query_start, key_start, head_count):
    token_rows = query_block.shape[0]
    key_count = window_block.shape[0]
    grouped = query_block.astype(jnp.float32).reshape(token_rows, head_count, HD)
    key_rows = window_block[:, :HD].astype(jnp.float32)
    value_rows = window_block[:, HD:].astype(jnp.float32)
    scores = jnp.einsum('qhd,kd->hqk', grouped, key_rows, precision=lax.Precision.HIGHEST) * HD ** (-0.5)
    query_pos = query_start + jnp.arange(token_rows, dtype=jnp.int32)
    key_pos = key_start + jnp.arange(key_count, dtype=jnp.int32)
    distance = query_pos[:, None] - key_pos[None, :]
    allowed = (distance >= 0) & (distance < WINDOW) & (key_pos[None, :] >= 0)
    scores = jnp.where(allowed[None], scores, masked_score)
    row_peak = lax.optimization_barrier(jnp.max(scores, axis=2, keepdims=True))
    weights = jnp.exp(scores - row_peak)
    softmax_probs = (weights / lax.optimization_barrier(jnp.sum(weights, axis=2, keepdims=True))).astype(jnp.bfloat16)
    output = jnp.einsum('hqk,kd->qhd', softmax_probs.astype(jnp.float32), value_rows, precision=lax.Precision.HIGHEST)
    return output.reshape(token_rows, head_count * HD).astype(jnp.bfloat16)

def reference(branch_in, branch_gate, conv_taps, conv_shift, inflow_weight, inflow_bias, decay_weight, decay_bias, decay_param, stream, norm_gain, memory_weight, queries):
    mixed_conv = convolve(branch_in, conv_taps, conv_shift)
    block_count = TOTAL_TOKENS // TOK_DEV
    inflow_full = inflow_weight.astype(jnp.float32)
    decay_full = decay_weight.astype(jnp.float32)
    softened = jax.nn.softplus(-decay_param)

    def run_block(carried, block_pair):
        conv_block, gate_block = block_pair
        conv_float = conv_block.astype(jnp.float32)
        grouped = conv_float.reshape(TOK_DEV, RHEADS, BLK)
        inflow = jax.nn.sigmoid(jnp.einsum('tnb,nbc->tnc', grouped, inflow_full, precision=lax.Precision.HIGHEST).reshape(TOK_DEV, R) + inflow_bias[None, :])
        recurrence = jax.nn.sigmoid(jnp.einsum('tnb,nbc->tnc', grouped, decay_full, precision=lax.Precision.HIGHEST).reshape(TOK_DEV, R) + decay_bias[None, :])
        log_decay = -decay_power * recurrence * softened[None, :]
        factor = jnp.exp(log_decay)
        pushed = jnp.sqrt(-jnp.expm1(2.0 * log_decay)) * inflow * conv_float

        def tick(current, entries):
            updated = entries[0] * current + entries[1]
            return (updated, updated)
        carried, history = lax.scan(tick, carried, (factor, pushed))
        output = (history * jax.nn.gelu(gate_block.astype(jnp.float32), approximate=True)).astype(jnp.bfloat16)
        return (carried, output)
    _, outputs = lax.scan(run_block, jnp.zeros((R,), jnp.float32), (mixed_conv.reshape(block_count, TOK_DEV, R), branch_gate.reshape(block_count, TOK_DEV, R)))
    recurrent_out = outputs.reshape(TOTAL_TOKENS, R)
    stream_float = stream.astype(jnp.float32)
    squares = lax.optimization_barrier(jnp.sum(jnp.square(stream_float), axis=1))
    scaled = (stream_float * norm_gain[None, :]).astype(jnp.bfloat16)
    raw_memory = jnp.dot(scaled, memory_weight, preferred_element_type=jnp.float32)
    memory = (raw_memory / jnp.sqrt(squares / D + norm_epsilon)[:, None]).astype(jnp.bfloat16)
    padded = jnp.concatenate([jnp.zeros((WINDOW, 2 * HD), jnp.bfloat16), memory], axis=0)

    def attend(block_index):
        block_start = (block_index * TOK_DEV).astype(jnp.int32)
        query_block = lax.dynamic_slice_in_dim(queries, block_start, TOK_DEV, 0)
        window_block = lax.dynamic_slice_in_dim(padded, block_start, WINDOW + TOK_DEV, 0)
        return attend_block(query_block, window_block, block_start, block_start - WINDOW, H)
    attended = lax.map(attend, jnp.arange(block_count, dtype=jnp.int32)).reshape(TOTAL_TOKENS, H * HD)
    return (recurrent_out, attended)
```

```python
import functools

import jax
import jax.numpy as jnp
from jax import lax
from jax.experimental import pallas as pl
from jax.experimental.pallas import tpu as pltpu
from jax.sharding import PartitionSpec as P

HD = 256
CONV = 4
WINDOW = 2048
BLK = 256
HALO = 16
CHUNK = 128
QROWS = 256
MESH = pl.DeviceIdType.MESH
F32 = jnp.float32
BF16 = jnp.bfloat16

decay_power = 8.0
norm_epsilon = 1e-06
masked_score = -1e30


def neg_expm1(x):
    series = 1.0 + x * (1.0 / 7.0)
    for k in (6.0, 5.0, 4.0, 3.0, 2.0):
        series = 1.0 + x * (1.0 / k) * series
    return jnp.where(x > -0.5, -x * series, 1.0 - jnp.exp(x))


def exchange_kernel(
    n, mp, back, far,
    taps, shift, ibias, dbias, dparam, gain,
    branch_h, gate_h, iw_h, dw_h, stream_h, mw_h,
    rec_out, kv,
    ext, gate, iw, dw, stream, mw, a_s, b_s, pairs,
    own, p_send, p_recv, ps_send, ps_recv, own_sq, y_send, y_recv, ys_send, ys_recv,
    lsem, esem, psem, ysem, csend, crecv, zs, zr, xs, xr, ds, dr,
):
    seq = lax.axis_index("seq")
    m = lax.axis_index("mp")
    core = lax.rem(m, 2)
    odd = lax.rem(seq, 2)
    mate = m + 1 - 2 * core
    T, C = rec_out.shape
    half = T // 2
    chunks = half // CHUNK
    groups = C // BLK
    peers = mp // 2
    own_base = core * half
    other_base = (1 - core) * half

    def local(src, dst, k):
        return pltpu.make_async_copy(src, dst, lsem.at[k])

    def rows(base, ch):
        return pl.ds(pl.multiple_of(base + ch * CHUNK, CHUNK), CHUNK)

    halves = [pl.ds(pl.multiple_of(b, CHUNK), half) for b in (other_base, own_base)]
    loads = [
        local(mw_h, mw, 0),
        local(stream_h.at[halves[0]], stream.at[halves[0]], 1),
        local(stream_h.at[halves[1]], stream.at[halves[1]], 2),
        local(branch_h, ext.at[pl.ds(HALO, T)], 3),
        local(iw_h, iw, 4),
        local(dw_h, dw, 5),
        local(gate_h, gate, 6),
    ]
    for load in loads:
        load.start()

    @pl.when(seq == 0)
    def _():
        ext[pl.ds(0, HALO), :] = jnp.zeros((HALO, C), BF16)

    for d in range(1, far + 1):
        @pl.when(seq < d)
        def _():
            kv[far - d] = jnp.zeros((T, kv.shape[2]), BF16)

    barrier = pltpu.get_barrier_semaphore()

    def greet(j, _):
        @pl.when(j != seq)
        def _():
            pl.semaphore_signal(barrier, inc=1, device_id=(j, m), device_id_type=MESH)
        return 0

    lax.fori_loop(0, n, greet, 0)
    for r in range(1, mp):
        pl.semaphore_signal(barrier, inc=1, device_id=(seq, lax.rem(m + r, mp)), device_id_type=MESH)
    pl.semaphore_wait(barrier, n - 1 + mp - 1)

    def remote(src, dst, ssem, rsem, to):
        return pltpu.make_async_remote_copy(
            src_ref=src, dst_ref=dst, send_sem=ssem, recv_sem=rsem, device_id=to, device_id_type=MESH
        )

    edge = remote(
        branch_h.at[pl.ds(T - HALO, HALO)], ext.at[pl.ds(0, HALO)], esem.at[0], esem.at[1], (seq + 1, m)
    )

    @pl.when(seq + 1 < n)
    def _():
        edge.start()

    def partial(base, ch):
        x = stream[rows(base, ch), :].astype(F32)
        square = jnp.sum(x * x, axis=1, keepdims=True)
        square = jnp.transpose(jnp.broadcast_to(square, (CHUNK, 128)))[:8]
        scaled = (x * gain[...]).astype(BF16)
        return jnp.dot(scaled, mw[...], preferred_element_type=F32), square

    def mate_copies(ch):
        return (
            remote(p_send.at[ch], p_recv.at[ch], psem.at[0, ch], psem.at[1, ch], (seq, mate)),
            remote(ps_send.at[ch], ps_recv.at[ch], psem.at[2, ch], psem.at[3, ch], (seq, mate)),
        )

    def peer_copies(r, ch):
        to = (seq, lax.rem(m + 2 * r, mp))
        return (
            remote(y_send.at[ch], y_recv.at[r - 1, ch], ysem.at[0, r - 1, ch], ysem.at[1, r - 1, ch], to),
            remote(ys_send.at[ch], ys_recv.at[r - 1, ch], ysem.at[2, r - 1, ch], ysem.at[3, r - 1, ch], to),
        )

    loads[0].wait()
    loads[1].wait()
    for ch in range(chunks):
        p_send[ch], ps_send[ch] = partial(other_base, ch)
        for copy in mate_copies(ch):
            copy.start()
    loads[2].wait()
    for ch in range(chunks):
        own[ch], own_sq[ch] = partial(own_base, ch)
    for ch in range(chunks):
        for copy in mate_copies(ch):
            copy.wait_recv()
        y_send[ch] = (own[ch] + p_recv[ch]).astype(BF16)
        ys_send[ch] = own_sq[ch] + ps_recv[ch]
        for r in range(1, peers):
            for copy in peer_copies(r, ch):
                copy.start()

    loads[3].wait()
    loads[4].wait()
    loads[5].wait()

    @pl.when(seq > 0)
    def _():
        edge.wait_recv()

    def gates(g, _):
        lanes = pl.ds(pl.multiple_of(g * BLK, BLK), BLK)
        soft = jnp.log1p(jnp.exp(-dparam[:, lanes]))
        row8 = lax.broadcasted_iota(jnp.int32, (1, 8, BLK), 1)

        def tile(t, _):
            x = ext[pl.ds(pl.multiple_of(t * CHUNK, CHUNK), CHUNK + HALO), lanes].astype(F32)
            total = shift[:, lanes] + taps[pl.ds(0, 1), lanes] * x[HALO:]
            for k in range(1, CONV):
                total = total + taps[pl.ds(k, 1), lanes] * pltpu.roll(x, k, 0)[HALO:]
            mixed = total.astype(BF16)
            inflow = jax.nn.sigmoid(jnp.dot(mixed, iw[g], preferred_element_type=F32) + ibias[:, lanes])
            rec = jax.nn.sigmoid(jnp.dot(mixed, dw[g], preferred_element_type=F32) + dbias[:, lanes])
            log_decay = (-decay_power * soft) * rec
            a = jnp.exp(log_decay)
            b = jnp.sqrt(neg_expm1(2.0 * log_decay)) * inflow * mixed.astype(F32)
            a = a.reshape(CHUNK // 8, 8, BLK)
            b = b.reshape(CHUNK // 8, 8, BLK)
            for k in (1, 2, 4):
                keep = row8 >= k
                b = b + a * jnp.where(keep, pltpu.roll(b, k, 1), 0.0)
                a = a * jnp.where(keep, pltpu.roll(a, k, 1), 1.0)
            here = pl.ds(pl.multiple_of(t * CHUNK, CHUNK), CHUNK)
            a_s[here, lanes] = a.reshape(CHUNK, BLK)
            b_s[here, lanes] = b.reshape(CHUNK, BLK)
            return 0

        lax.fori_loop(0, T // CHUNK, tile, 0)
        return 0

    lax.fori_loop(0, groups // 2, gates, 0)

    def z_copy(d, ch):
        at = rows(own_base, ch)
        return remote(kv.at[far - d, at], kv.at[far - d - 2, at], zs.at[d, ch], zr.at[d + 2, ch], (seq + 2, m))

    def z_arrival(d, ch):
        at = rows(own_base, ch)
        return remote(kv.at[far - d, at], kv.at[far - d, at], zs.at[d, ch], zr.at[d, ch], (seq, mate))

    def x_copy(d, e, ch):
        at = rows(own_base, ch)
        return remote(
            kv.at[far - d, at], kv.at[far - e, at], xs.at[d, ch], xr.at[e, ch], (seq + (e - d), m)
        )

    def x_arrival(d, ch):
        at = rows(own_base, ch)
        return remote(kv.at[far - d, at], kv.at[far - d, at], xs.at[d, ch], xr.at[d, ch], (seq, mate))

    def d_copy(d, ch):
        at = rows(own_base, ch)
        return remote(kv.at[far - d, at], kv.at[far - d, at], ds.at[d, ch], dr.at[d, ch], (seq, mate))

    def d_arrival(d, ch):
        at = rows(other_base, ch)
        return remote(kv.at[far - d, at], kv.at[far - d, at], ds.at[d, ch], dr.at[d, ch], (seq, mate))

    def even_copies(d, ch, act):
        if d + 2 <= far:
            @pl.when((seq >= d) & (seq + 2 < n))
            def _():
                act(z_copy(d, ch))
        if d >= 2:
            @pl.when((seq >= d) & (odd == 1))
            def _():
                act(x_copy(d, d - 1, ch))
        if d + 1 <= back:
            @pl.when((seq >= d) & (odd == 0))
            def _():
                act(x_copy(d, d + 1, ch))

    def mate_out(d, ch, act):
        if d <= back:
            @pl.when(seq >= d)
            def _():
                act(d_copy(d, ch))

    start = lambda copy: copy.start()
    features = C * mp
    for ch in range(chunks):
        for r in range(1, peers):
            for copy in peer_copies(r, ch):
                copy.wait_recv()
        total = y_send[ch].astype(F32)
        square = ys_send[ch]
        for r in range(1, peers):
            total = total + y_recv[r - 1, ch].astype(F32)
            square = square + ys_recv[r - 1, ch]
        inverse = 1.0 / jnp.sqrt(square / features + norm_epsilon)
        inverse = jnp.transpose(jnp.broadcast_to(inverse[:1], (128, CHUNK)))
        kv[far, rows(own_base, ch), :] = (total * inverse[:, :1]).astype(BF16)
        even_copies(0, ch, start)
        mate_out(0, ch, start)

    lax.fori_loop(groups // 2, groups, gates, 0)

    def carry_rows(j, state):
        factor, value = state
        at = pl.ds(pl.multiple_of(j * 8, 8), 8)
        a = a_s[at, :]
        b = b_s[at, :] + a * value
        a = a * factor
        a_s[at, :] = a
        b_s[at, :] = b
        return jnp.broadcast_to(a[7:8], (8, C)), jnp.broadcast_to(b[7:8], (8, C))

    factor, value = lax.fori_loop(0, T // 8, carry_rows, (jnp.ones((8, C), F32), jnp.zeros((8, C), F32)))
    pairs[seq, pl.ds(0, 1), :] = factor[:1]
    pairs[seq, pl.ds(1, 1), :] = value[:1]

    def pair_copy(j):
        return remote(pairs.at[seq], pairs.at[seq], csend.at[j], crecv.at[seq], (j, m))

    def pair_arrival(j):
        return remote(pairs.at[j], pairs.at[j], csend.at[j], crecv.at[j], (seq, mate))

    def send_pair(j, _):
        pair_copy(j).start()
        return 0

    lax.fori_loop(seq + 1, n, send_pair, 0)

    def forward(d):
        for ch in range(chunks):
            @pl.when(seq >= d)
            def _():
                z_arrival(d, ch).wait_recv()
            even_copies(d, ch, start)
            mate_out(d, ch, start)

    if far >= 2:
        forward(2)

    loads[6].wait()

    def join(j, incoming):
        pair_arrival(j).wait_recv()
        return pairs[j, pl.ds(0, 1), :] * incoming + pairs[j, pl.ds(1, 1), :]

    incoming = lax.fori_loop(0, seq, join, jnp.zeros((1, C), F32))

    def finish(j, _):
        at = pl.ds(pl.multiple_of(j * 16, 16), 16)
        states = b_s[at, :] + a_s[at, :] * incoming
        v = gate[at, :].astype(F32)
        gelu = 0.5 * v * (1.0 + jnp.tanh(0.7978845608028654 * (v + 0.044715 * v * v * v)))
        rec_out[at, :] = (states * gelu).astype(BF16)
        return 0

    lax.fori_loop(0, T // 16, finish, 0)

    for d in range(4, far + 1, 2):
        forward(d)
    for d in range(1, back + 1, 2):
        for ch in range(chunks):
            @pl.when(seq >= d)
            def _():
                x_arrival(d, ch).wait_recv()
            mate_out(d, ch, start)

    for d in range(back + 1):
        for ch in range(chunks):
            @pl.when(seq >= d)
            def _():
                d_arrival(d, ch).wait_recv()
    sent = lambda copy: copy.wait_send()
    for ch in range(chunks):
        for copy in mate_copies(ch):
            copy.wait_send()
        for r in range(1, peers):
            for copy in peer_copies(r, ch):
                copy.wait_send()
        for d in range(0, far + 1, 2):
            even_copies(d, ch, sent)
        for d in range(back + 1):
            mate_out(d, ch, sent)

    @pl.when(seq + 1 < n)
    def _():
        edge.wait_send()

    def pair_sent(j, _):
        pair_copy(j).wait_send()
        return 0

    lax.fori_loop(seq + 1, n, pair_sent, 0)


def attend_kernel(back, T, q_ref, kv_ref, out_ref, s_ref):
    seq = lax.axis_index("seq")
    first = pl.program_id(1) * QROWS
    steps = WINDOW // QROWS + 1
    q = q_ref[...]
    scale = HD ** (-0.5)
    row = lax.broadcasted_iota(jnp.int32, (QROWS, QROWS), 0)
    col = lax.broadcasted_iota(jnp.int32, (QROWS, QROWS), 1)
    peak = jnp.full((QROWS, QROWS), masked_score, F32)
    for k in range(steps):
        at = first + k * QROWS
        keys = kv_ref[pl.ds(pl.multiple_of(at, QROWS), QROWS), pl.ds(0, HD)]
        s = lax.dot_general(q, keys, (((1,), (1,)), ((), ())), preferred_element_type=F32) * scale
        if k == 0:
            s = jnp.where(col > row, s, masked_score)
        if k == steps - 1:
            s = jnp.where(col <= row, s, masked_score)
        else:
            s = jnp.where(at >= (back - seq) * T, s, masked_score)
        s_ref[:, pl.ds(k * QROWS, QROWS)] = s
        peak = jnp.maximum(peak, s)
    peak = jnp.max(peak, axis=1, keepdims=True)
    total = jnp.zeros((QROWS, QROWS), F32)
    acc = jnp.zeros((QROWS, HD), F32)
    for k in range(steps):
        p = jnp.exp(s_ref[:, pl.ds(k * QROWS, QROWS)] - peak)
        total = total + p
        values = kv_ref[pl.ds(pl.multiple_of(first + k * QROWS, QROWS), QROWS), pl.ds(HD, HD)]
        acc = acc + jnp.dot(p.astype(BF16), values, preferred_element_type=F32)
    out_ref[...] = (acc / jnp.sum(total, axis=1, keepdims=True)).astype(BF16)


def shards(
    n, mp,
    branch_in, branch_gate, conv_taps, conv_shift, inflow_weight, inflow_bias, decay_weight, decay_bias,
    decay_param, stream, norm_gain, memory_weight, queries,
):
    T, C = branch_in.shape
    width = memory_weight.shape[1]
    back = WINDOW // T
    far = back + back % 2
    chunks = T // 2 // CHUNK
    groups = inflow_weight.shape[0]
    peers = mp // 2
    vmem = pl.BlockSpec(memory_space=pltpu.VMEM)
    hbm = pl.BlockSpec(memory_space=pl.ANY)
    dma = pltpu.SemaphoreType.DMA
    flat = lambda v: v.reshape(1, -1)
    others = max(peers - 1, 1)
    recurrent_out, kv = pl.pallas_call(
        functools.partial(exchange_kernel, n, mp, back, far),
        out_shape=(
            jax.ShapeDtypeStruct((T, C), BF16),
            jax.ShapeDtypeStruct((far + 1, T, width), BF16),
        ),
        in_specs=[vmem] * 6 + [hbm] * 6,
        out_specs=(vmem, vmem),
        scratch_shapes=[
            pltpu.VMEM((T + HALO, C), BF16),
            pltpu.VMEM((T, C), BF16),
            pltpu.VMEM((groups, BLK, BLK), BF16),
            pltpu.VMEM((groups, BLK, BLK), BF16),
            pltpu.VMEM((T, C), BF16),
            pltpu.VMEM((C, width), BF16),
            pltpu.VMEM((T, C), F32),
            pltpu.VMEM((T, C), F32),
            pltpu.VMEM((n, 2, C), F32),
            pltpu.VMEM((chunks, CHUNK, width), F32),
            pltpu.VMEM((chunks, CHUNK, width), F32),
            pltpu.VMEM((chunks, CHUNK, width), F32),
            pltpu.VMEM((chunks, 8, CHUNK), F32),
            pltpu.VMEM((chunks, 8, CHUNK), F32),
            pltpu.VMEM((chunks, 8, CHUNK), F32),
            pltpu.VMEM((chunks, CHUNK, width), BF16),
            pltpu.VMEM((others, chunks, CHUNK, width), BF16),
            pltpu.VMEM((chunks, 8, CHUNK), F32),
            pltpu.VMEM((others, chunks, 8, CHUNK), F32),
            dma((7,)),
            dma((2,)),
            dma((4, chunks)),
            dma((4, others, chunks)),
            dma((n,)),
            dma((n,)),
        ]
        + [dma((far + 3, chunks))] * 6,
        compiler_params=pltpu.CompilerParams(collective_id=0, has_side_effects=True),
    )(
        conv_taps, flat(conv_shift), flat(inflow_bias), flat(decay_bias), flat(decay_param), flat(norm_gain),
        branch_in, branch_gate, inflow_weight, decay_weight, stream, memory_weight,
    )
    window = kv[far - back:].reshape((back + 1) * T, width)
    heads = queries.shape[1] // HD
    attended = pl.pallas_call(
        functools.partial(attend_kernel, back, T),
        out_shape=jax.ShapeDtypeStruct(queries.shape, BF16),
        grid=(heads, T // QROWS),
        in_specs=[
            pl.BlockSpec((QROWS, HD), lambda h, i: (i, h)),
            pl.BlockSpec(window.shape, lambda h, i: (0, 0)),
        ],
        out_specs=pl.BlockSpec((QROWS, HD), lambda h, i: (i, h)),
        scratch_shapes=[pltpu.VMEM((QROWS, WINDOW + QROWS), F32)],
    )(queries, window)
    return recurrent_out, attended


def solution(mesh):
    return jax.shard_map(
        functools.partial(shards, mesh.shape["seq"], mesh.shape["mp"]),
        mesh=mesh,
        in_specs=(
            P("seq", "mp"),
            P("seq", "mp"),
            P(None, "mp"),
            P("mp"),
            P("mp", None, None),
            P("mp"),
            P("mp", None, None),
            P("mp"),
            P("mp"),
            P("seq", "mp"),
            P("mp"),
            P("mp", None),
            P("seq", "mp"),
        ),
        out_specs=(P("seq", "mp"), P("seq", "mp")),
        check_vma=False,
    )
```

```python
import functools

import jax
import jax.numpy as jnp
from jax import lax
from jax.experimental import pallas as pl
from jax.experimental.pallas import tpu as pltpu
from jax.sharding import PartitionSpec as P

HD = 256
CONV = 4
WINDOW = 2048
BLK = 256
HALO = 16
CHUNK = 128
QROWS = 256
MESH = pl.DeviceIdType.MESH
F32 = jnp.float32
BF16 = jnp.bfloat16

decay_power = 8.0
norm_epsilon = 1e-06
masked_score = -1e30


def neg_expm1(x):
    series = 1.0 + x * (1.0 / 7.0)
    for k in (6.0, 5.0, 4.0, 3.0, 2.0):
        series = 1.0 + x * (1.0 / k) * series
    return jnp.where(x > -0.5, -x * series, 1.0 - jnp.exp(x))


def exchange_kernel(
    n, mp, back, far,
    taps, shift, ibias, dbias, dparam, gain,
    branch_h, gate_h, iw_h, dw_h, stream_h, mw_h, q_h,
    rec_out, att_out,
    kv, q_v, acc_s, peak_s, sum_s,
    ext, gate, iw, dw, stream, mw, a_s, b_s, pairs,
    own, p_send, p_recv, ps_send, ps_recv, own_sq, y_send, y_recv, ys_send, ys_recv,
    lsem, esem, psem, ysem, csend, crecv, zs, zr, xs, xr, ds, dr,
):
    seq = lax.axis_index("seq")
    m = lax.axis_index("mp")
    core = lax.rem(m, 2)
    odd = lax.rem(seq, 2)
    mate = m + 1 - 2 * core
    T, C = rec_out.shape
    half = T // 2
    chunks = half // CHUNK
    groups = C // BLK
    peers = mp // 2
    own_base = core * half
    other_base = (1 - core) * half

    def local(src, dst, k):
        return pltpu.make_async_copy(src, dst, lsem.at[k])

    def rows(base, ch):
        return pl.ds(pl.multiple_of(base + ch * CHUNK, CHUNK), CHUNK)

    halves = [pl.ds(pl.multiple_of(b, CHUNK), half) for b in (other_base, own_base)]
    loads = [
        local(mw_h, mw, 0),
        local(stream_h.at[halves[0]], stream.at[halves[0]], 1),
        local(stream_h.at[halves[1]], stream.at[halves[1]], 2),
        local(branch_h, ext.at[pl.ds(HALO, T)], 3),
        local(iw_h, iw, 4),
        local(dw_h, dw, 5),
        local(gate_h, gate, 6),
        local(q_h, q_v, 7),
    ]
    for load in loads:
        load.start()

    @pl.when(seq == 0)
    def _():
        ext[pl.ds(0, HALO), :] = jnp.zeros((HALO, C), BF16)

    barrier = pltpu.get_barrier_semaphore()

    def greet(j, _):
        @pl.when(j != seq)
        def _():
            pl.semaphore_signal(barrier, inc=1, device_id=(j, m), device_id_type=MESH)
        return 0

    lax.fori_loop(0, n, greet, 0)
    for r in range(1, mp):
        pl.semaphore_signal(barrier, inc=1, device_id=(seq, lax.rem(m + r, mp)), device_id_type=MESH)
    pl.semaphore_wait(barrier, n - 1 + mp - 1)

    def remote(src, dst, ssem, rsem, to):
        return pltpu.make_async_remote_copy(
            src_ref=src, dst_ref=dst, send_sem=ssem, recv_sem=rsem, device_id=to, device_id_type=MESH
        )

    edge = remote(
        branch_h.at[pl.ds(T - HALO, HALO)], ext.at[pl.ds(0, HALO)], esem.at[0], esem.at[1], (seq + 1, m)
    )

    @pl.when(seq + 1 < n)
    def _():
        edge.start()

    def partial(base, ch):
        x = stream[rows(base, ch), :].astype(F32)
        square = jnp.sum(x * x, axis=1, keepdims=True)
        square = jnp.transpose(jnp.broadcast_to(square, (CHUNK, 128)))[:8]
        scaled = (x * gain[...]).astype(BF16)
        return jnp.dot(scaled, mw[...], preferred_element_type=F32), square

    def mate_copies(ch):
        return (
            remote(p_send.at[ch], p_recv.at[ch], psem.at[0, ch], psem.at[1, ch], (seq, mate)),
            remote(ps_send.at[ch], ps_recv.at[ch], psem.at[2, ch], psem.at[3, ch], (seq, mate)),
        )

    def peer_copies(r, ch):
        to = (seq, lax.rem(m + 2 * r, mp))
        return (
            remote(y_send.at[ch], y_recv.at[r - 1, ch], ysem.at[0, r - 1, ch], ysem.at[1, r - 1, ch], to),
            remote(ys_send.at[ch], ys_recv.at[r - 1, ch], ysem.at[2, r - 1, ch], ysem.at[3, r - 1, ch], to),
        )

    loads[0].wait()
    loads[1].wait()
    for ch in range(chunks):
        p_send[ch], ps_send[ch] = partial(other_base, ch)
        for copy in mate_copies(ch):
            copy.start()
    loads[2].wait()
    for ch in range(chunks):
        own[ch], own_sq[ch] = partial(own_base, ch)
    for ch in range(chunks):
        for copy in mate_copies(ch):
            copy.wait_recv()
        y_send[ch] = (own[ch] + p_recv[ch]).astype(BF16)
        ys_send[ch] = own_sq[ch] + ps_recv[ch]
        for r in range(1, peers):
            for copy in peer_copies(r, ch):
                copy.start()

    loads[3].wait()
    loads[4].wait()
    loads[5].wait()

    @pl.when(seq > 0)
    def _():
        edge.wait_recv()

    def gates(g, _):
        lanes = pl.ds(pl.multiple_of(g * BLK, BLK), BLK)
        soft = jnp.log1p(jnp.exp(-dparam[:, lanes]))
        row8 = lax.broadcasted_iota(jnp.int32, (1, 8, BLK), 1)

        def tile(t, _):
            x = ext[pl.ds(pl.multiple_of(t * CHUNK, CHUNK), CHUNK + HALO), lanes].astype(F32)
            total = shift[:, lanes] + taps[pl.ds(0, 1), lanes] * x[HALO:]
            for k in range(1, CONV):
                total = total + taps[pl.ds(k, 1), lanes] * pltpu.roll(x, k, 0)[HALO:]
            mixed = total.astype(BF16)
            inflow = jax.nn.sigmoid(jnp.dot(mixed, iw[g], preferred_element_type=F32) + ibias[:, lanes])
            rec = jax.nn.sigmoid(jnp.dot(mixed, dw[g], preferred_element_type=F32) + dbias[:, lanes])
            log_decay = (-decay_power * soft) * rec
            a = jnp.exp(log_decay)
            b = jnp.sqrt(neg_expm1(2.0 * log_decay)) * inflow * mixed.astype(F32)
            a = a.reshape(CHUNK // 8, 8, BLK)
            b = b.reshape(CHUNK // 8, 8, BLK)
            for k in (1, 2, 4):
                keep = row8 >= k
                b = b + a * jnp.where(keep, pltpu.roll(b, k, 1), 0.0)
                a = a * jnp.where(keep, pltpu.roll(a, k, 1), 1.0)
            here = pl.ds(pl.multiple_of(t * CHUNK, CHUNK), CHUNK)
            a_s[here, lanes] = a.reshape(CHUNK, BLK)
            b_s[here, lanes] = b.reshape(CHUNK, BLK)
            return 0

        lax.fori_loop(0, T // CHUNK, tile, 0)
        return 0

    lax.fori_loop(0, groups // 2, gates, 0)

    def z_copy(d, ch):
        at = rows(own_base, ch)
        return remote(kv.at[far - d, at], kv.at[far - d - 2, at], zs.at[d, ch], zr.at[d + 2, ch], (seq + 2, m))

    def z_arrival(d, ch):
        at = rows(own_base, ch)
        return remote(kv.at[far - d, at], kv.at[far - d, at], zs.at[d, ch], zr.at[d, ch], (seq, mate))

    def x_copy(d, e, ch):
        at = rows(own_base, ch)
        return remote(
            kv.at[far - d, at], kv.at[far - e, at], xs.at[d, ch], xr.at[e, ch], (seq + (e - d), m)
        )

    def x_arrival(d, ch):
        at = rows(own_base, ch)
        return remote(kv.at[far - d, at], kv.at[far - d, at], xs.at[d, ch], xr.at[d, ch], (seq, mate))

    def d_copy(d, ch):
        at = rows(own_base, ch)
        return remote(kv.at[far - d, at], kv.at[far - d, at], ds.at[d, ch], dr.at[d, ch], (seq, mate))

    def d_arrival(d, ch):
        at = rows(other_base, ch)
        return remote(kv.at[far - d, at], kv.at[far - d, at], ds.at[d, ch], dr.at[d, ch], (seq, mate))

    def even_copies(d, ch, act):
        if d + 2 <= far:
            @pl.when((seq >= d) & (seq + 2 < n))
            def _():
                act(z_copy(d, ch))
        if d >= 2:
            @pl.when((seq >= d) & (odd == 1))
            def _():
                act(x_copy(d, d - 1, ch))
        if d + 1 <= back:
            @pl.when((seq >= d) & (odd == 0))
            def _():
                act(x_copy(d, d + 1, ch))

    def mate_out(d, ch, act):
        if d <= back:
            @pl.when(seq >= d)
            def _():
                act(d_copy(d, ch))

    start = lambda copy: copy.start()
    features = C * mp
    for ch in range(chunks):
        for r in range(1, peers):
            for copy in peer_copies(r, ch):
                copy.wait_recv()
        total = y_send[ch].astype(F32)
        square = ys_send[ch]
        for r in range(1, peers):
            total = total + y_recv[r - 1, ch].astype(F32)
            square = square + ys_recv[r - 1, ch]
        inverse = 1.0 / jnp.sqrt(square / features + norm_epsilon)
        inverse = jnp.transpose(jnp.broadcast_to(inverse[:1], (128, CHUNK)))
        kv[far, rows(own_base, ch), :] = (total * inverse[:, :1]).astype(BF16)
        even_copies(0, ch, start)
        mate_out(0, ch, start)

    lax.fori_loop(groups // 2, groups, gates, 0)

    def carry_rows(j, state):
        factor, value = state
        at = pl.ds(pl.multiple_of(j * 8, 8), 8)
        a = a_s[at, :]
        b = b_s[at, :] + a * value
        a = a * factor
        a_s[at, :] = a
        b_s[at, :] = b
        return jnp.broadcast_to(a[7:8], (8, C)), jnp.broadcast_to(b[7:8], (8, C))

    factor, value = lax.fori_loop(0, T // 8, carry_rows, (jnp.ones((8, C), F32), jnp.zeros((8, C), F32)))
    pairs[seq, pl.ds(0, 1), :] = factor[:1]
    pairs[seq, pl.ds(1, 1), :] = value[:1]

    def pair_copy(j):
        return remote(pairs.at[seq], pairs.at[seq], csend.at[j], crecv.at[seq], (j, m))

    def pair_arrival(j):
        return remote(pairs.at[j], pairs.at[j], csend.at[j], crecv.at[j], (seq, mate))

    def send_pair(j, _):
        pair_copy(j).start()
        return 0

    lax.fori_loop(seq + 1, n, send_pair, 0)

    def forward(d):
        for ch in range(chunks):
            @pl.when(seq >= d)
            def _():
                z_arrival(d, ch).wait_recv()
            even_copies(d, ch, start)
            mate_out(d, ch, start)

    loads[7].wait()

    def scale_rows(j, _):
        at = pl.ds(pl.multiple_of(j * 64, 64), 64)
        q_v[at, :] = (q_v[at, :].astype(F32) * HD ** (-0.5)).astype(BF16)
        return 0

    lax.fori_loop(0, T // 64, scale_rows, 0)
    if far >= 2:
        forward(2)

    row = lax.broadcasted_iota(jnp.int32, (QROWS, QROWS), 0)
    col = lax.broadcasted_iota(jnp.int32, (QROWS, QROWS), 1)
    tiles = T // QROWS
    heads = q_v.shape[1] // HD

    def attend_tile(d, h, i):
        unit = h * tiles + i
        low, high = 0, T
        if d == 0:
            high = (i + 1) * QROWS
        if d == back:
            low = i * QROWS
        q = q_v[pl.ds(i * QROWS, QROWS), pl.ds(pl.multiple_of(h * HD, HD), HD)]
        keys = kv[far - d, pl.ds(low, high - low), pl.ds(0, HD)]
        values = kv[far - d, pl.ds(low, high - low), pl.ds(HD, HD)]
        s = lax.dot_general(q, keys, (((1,), (1,)), ((), ())), preferred_element_type=F32)
        parts = [s[:, k : k + QROWS] for k in range(0, high - low, QROWS)]
        if d == 0:
            parts[-1] = jnp.where(col <= row, parts[-1], masked_score)
        if d == back:
            parts[0] = jnp.where(col > row, parts[0], masked_score)
        peak = functools.reduce(jnp.maximum, parts)
        peak = jnp.max(peak, axis=1, keepdims=True)
        if d > 0:
            before = peak_s[unit][:, :1]
            peak = jnp.maximum(before, peak)
            alpha = jnp.exp(before - peak)
        parts = [jnp.exp(part - peak) for part in parts]
        summed = sum(part[:, k : k + 128] for part in parts for k in range(0, QROWS, 128))
        p = jnp.concatenate([part.astype(BF16) for part in parts], axis=1)
        gathered = jnp.dot(p, values, preferred_element_type=F32)
        if d > 0:
            summed = summed + alpha * sum_s[unit]
            gathered = gathered + alpha * acc_s[unit]
        peak_s[unit] = jnp.broadcast_to(peak, (QROWS, 128))
        sum_s[unit] = summed
        acc_s[unit] = gathered

    def attend(d):
        if d > back:
            return

        @pl.when(seq >= d)
        def _():
            for ch in range(chunks):
                d_arrival(d, ch).wait_recv()

            def head(h, _):
                for i in range(tiles):
                    attend_tile(d, h, i)
                return 0

            lax.fori_loop(0, heads, head, 0)

    def crossed(d):
        for ch in range(chunks):
            @pl.when(seq >= d)
            def _():
                x_arrival(d, ch).wait_recv()
            mate_out(d, ch, start)

    def join(j, incoming):
        pair_arrival(j).wait_recv()
        return pairs[j, pl.ds(0, 1), :] * incoming + pairs[j, pl.ds(1, 1), :]

    def finish_recurrence():
        incoming = lax.fori_loop(0, seq, join, jnp.zeros((1, C), F32))

        def finish(j, _):
            at = pl.ds(pl.multiple_of(j * 16, 16), 16)
            states = b_s[at, :] + a_s[at, :] * incoming
            v = gate[at, :].astype(F32)
            gelu = 0.5 * v * (1.0 + jnp.tanh(0.7978845608028654 * (v + 0.044715 * v * v * v)))
            rec_out[at, :] = (states * gelu).astype(BF16)
            return 0

        lax.fori_loop(0, T // 16, finish, 0)

    attend(0)
    for d in range(2, far + 1, 2):
        crossed(d - 1)
        if d == 2:
            loads[6].wait()
            finish_recurrence()
        attend(d)
        if d + 2 <= far:
            forward(d + 2)
        attend(d - 1)

    def settle(h, _):
        for i in range(tiles):
            unit = h * tiles + i
            scale = 1.0 / jnp.sum(sum_s[unit], axis=1, keepdims=True)
            at = (pl.ds(i * QROWS, QROWS), pl.ds(pl.multiple_of(h * HD, HD), HD))
            att_out[at] = (acc_s[unit] * scale).astype(BF16)
        return 0

    lax.fori_loop(0, heads, settle, 0)

    sent = lambda copy: copy.wait_send()
    for ch in range(chunks):
        for copy in mate_copies(ch):
            copy.wait_send()
        for r in range(1, peers):
            for copy in peer_copies(r, ch):
                copy.wait_send()
        for d in range(0, far + 1, 2):
            even_copies(d, ch, sent)
        for d in range(back + 1):
            mate_out(d, ch, sent)

    @pl.when(seq + 1 < n)
    def _():
        edge.wait_send()

    def pair_sent(j, _):
        pair_copy(j).wait_send()
        return 0

    lax.fori_loop(seq + 1, n, pair_sent, 0)


def shards(
    n, mp,
    branch_in, branch_gate, conv_taps, conv_shift, inflow_weight, inflow_bias, decay_weight, decay_bias,
    decay_param, stream, norm_gain, memory_weight, queries,
):
    T, C = branch_in.shape
    width = memory_weight.shape[1]
    back = WINDOW // T
    far = back + back % 2
    chunks = T // 2 // CHUNK
    groups = inflow_weight.shape[0]
    peers = mp // 2
    vmem = pl.BlockSpec(memory_space=pltpu.VMEM)
    hbm = pl.BlockSpec(memory_space=pl.ANY)
    dma = pltpu.SemaphoreType.DMA
    flat = lambda v: v.reshape(1, -1)
    others = max(peers - 1, 1)
    heads = queries.shape[1] // HD
    units = heads * (T // QROWS)
    return pl.pallas_call(
        functools.partial(exchange_kernel, n, mp, back, far),
        out_shape=(
            jax.ShapeDtypeStruct((T, C), BF16),
            jax.ShapeDtypeStruct(queries.shape, BF16),
        ),
        in_specs=[vmem] * 6 + [hbm] * 7,
        out_specs=(vmem, vmem),
        scratch_shapes=[
            pltpu.VMEM((far + 1, T, width), BF16),
            pltpu.VMEM(queries.shape, BF16),
            pltpu.VMEM((units, QROWS, HD), F32),
            pltpu.VMEM((units, QROWS, 128), F32),
            pltpu.VMEM((units, QROWS, 128), F32),
            pltpu.VMEM((T + HALO, C), BF16),
            pltpu.VMEM((T, C), BF16),
            pltpu.VMEM((groups, BLK, BLK), BF16),
            pltpu.VMEM((groups, BLK, BLK), BF16),
            pltpu.VMEM((T, C), BF16),
            pltpu.VMEM((C, width), BF16),
            pltpu.VMEM((T, C), F32),
            pltpu.VMEM((T, C), F32),
            pltpu.VMEM((n, 2, C), F32),
            pltpu.VMEM((chunks, CHUNK, width), F32),
            pltpu.VMEM((chunks, CHUNK, width), F32),
            pltpu.VMEM((chunks, CHUNK, width), F32),
            pltpu.VMEM((chunks, 8, CHUNK), F32),
            pltpu.VMEM((chunks, 8, CHUNK), F32),
            pltpu.VMEM((chunks, 8, CHUNK), F32),
            pltpu.VMEM((chunks, CHUNK, width), BF16),
            pltpu.VMEM((others, chunks, CHUNK, width), BF16),
            pltpu.VMEM((chunks, 8, CHUNK), F32),
            pltpu.VMEM((others, chunks, 8, CHUNK), F32),
            dma((8,)),
            dma((2,)),
            dma((4, chunks)),
            dma((4, others, chunks)),
            dma((n,)),
            dma((n,)),
        ]
        + [dma((far + 3, chunks))] * 6,
        compiler_params=pltpu.CompilerParams(collective_id=0, has_side_effects=True),
    )(
        conv_taps, flat(conv_shift), flat(inflow_bias), flat(decay_bias), flat(decay_param), flat(norm_gain),
        branch_in, branch_gate, inflow_weight, decay_weight, stream, memory_weight, queries,
    )


def solution(mesh):
    return jax.shard_map(
        functools.partial(shards, mesh.shape["seq"], mesh.shape["mp"]),
        mesh=mesh,
        in_specs=(
            P("seq", "mp"),
            P("seq", "mp"),
            P(None, "mp"),
            P("mp"),
            P("mp", None, None),
            P("mp"),
            P("mp", None, None),
            P("mp"),
            P("mp"),
            P("seq", "mp"),
            P("mp"),
            P("mp", None),
            P("seq", "mp"),
        ),
        out_specs=(P("seq", "mp"), P("seq", "mp")),
        check_vma=False,
    )
```

```python
import functools

import jax
import jax.numpy as jnp
from jax import lax
from jax.experimental import pallas as pl
from jax.experimental.pallas import tpu as pltpu
from jax.sharding import PartitionSpec as P

HD = 256
CONV = 4
WINDOW = 2048
BLK = 256
HALO = 16
CHUNK = 128
QROWS = 256
MESH = pl.DeviceIdType.MESH
F32 = jnp.float32
BF16 = jnp.bfloat16

decay_power = 8.0
norm_epsilon = 1e-06
masked_score = -1e30


def neg_expm1(x):
    series = 1.0 + x * (1.0 / 7.0)
    for k in (6.0, 5.0, 4.0, 3.0, 2.0):
        series = 1.0 + x * (1.0 / k) * series
    return jnp.where(x > -0.5, -x * series, 1.0 - jnp.exp(x))


def exchange_kernel(
    n, mp, back, far,
    taps, shift, ibias, dbias, dparam, gain,
    branch_h, gate_h, iw_h, dw_h, stream_h, mw_h, q_h,
    rec_out, att_out,
    kv, q_v, acc_s, peak_s, sum_s,
    ext, gate, iw, dw, stream, mw, a_s, b_s, pairs,
    own, p_send, p_recv, ps_send, ps_recv, own_sq, y_send, y_recv, ys_send, ys_recv,
    lsem, esem, psem, ysem, csend, crecv, zs, zr, xs, xr, ds, dr,
):
    seq = lax.axis_index("seq")
    m = lax.axis_index("mp")
    core = lax.rem(m, 2)
    odd = lax.rem(seq, 2)
    mate = m + 1 - 2 * core
    T, C = rec_out.shape
    half = T // 2
    chunks = half // CHUNK
    groups = C // BLK
    peers = mp // 2
    own_base = core * half
    other_base = (1 - core) * half

    def local(src, dst, k):
        return pltpu.make_async_copy(src, dst, lsem.at[k])

    def rows(base, ch):
        return pl.ds(pl.multiple_of(base + ch * CHUNK, CHUNK), CHUNK)

    halves = [pl.ds(pl.multiple_of(b, CHUNK), half) for b in (other_base, own_base)]
    loads = [
        local(mw_h, mw, 0),
        local(stream_h.at[halves[0]], stream.at[halves[0]], 1),
        local(stream_h.at[halves[1]], stream.at[halves[1]], 2),
        local(branch_h, ext.at[pl.ds(HALO, T)], 3),
        local(iw_h, iw, 4),
        local(dw_h, dw, 5),
        local(gate_h, gate, 6),
        local(q_h, q_v, 7),
    ]
    for load in loads:
        load.start()

    @pl.when(seq == 0)
    def _():
        ext[pl.ds(0, HALO), :] = jnp.zeros((HALO, C), BF16)

    barrier = pltpu.get_barrier_semaphore()

    def greet(j, _):
        @pl.when(j != seq)
        def _():
            pl.semaphore_signal(barrier, inc=1, device_id=(j, m), device_id_type=MESH)
        return 0

    lax.fori_loop(0, n, greet, 0)
    for r in range(1, mp):
        pl.semaphore_signal(barrier, inc=1, device_id=(seq, lax.rem(m + r, mp)), device_id_type=MESH)
    pl.semaphore_wait(barrier, n - 1 + mp - 1)

    def remote(src, dst, ssem, rsem, to):
        return pltpu.make_async_remote_copy(
            src_ref=src, dst_ref=dst, send_sem=ssem, recv_sem=rsem, device_id=to, device_id_type=MESH
        )

    edge = remote(
        branch_h.at[pl.ds(T - HALO, HALO)], ext.at[pl.ds(0, HALO)], esem.at[0], esem.at[1], (seq + 1, m)
    )

    @pl.when(seq + 1 < n)
    def _():
        edge.start()

    def partial(base, ch):
        x = stream[rows(base, ch), :].astype(F32)
        square = jnp.sum(x * x, axis=1, keepdims=True)
        square = jnp.transpose(jnp.broadcast_to(square, (CHUNK, 128)))[:8]
        scaled = (x * gain[...]).astype(BF16)
        return jnp.dot(scaled, mw[...], preferred_element_type=F32), square

    def mate_copies(ch):
        return (
            remote(p_send.at[ch], p_recv.at[ch], psem.at[0, ch], psem.at[1, ch], (seq, mate)),
            remote(ps_send.at[ch], ps_recv.at[ch], psem.at[2, ch], psem.at[3, ch], (seq, mate)),
        )

    def peer_copies(r, ch):
        to = (seq, lax.rem(m + 2 * r, mp))
        return (
            remote(y_send.at[ch], y_recv.at[r - 1, ch], ysem.at[0, r - 1, ch], ysem.at[1, r - 1, ch], to),
            remote(ys_send.at[ch], ys_recv.at[r - 1, ch], ysem.at[2, r - 1, ch], ysem.at[3, r - 1, ch], to),
        )

    loads[0].wait()
    loads[1].wait()
    for ch in range(chunks):
        p_send[ch], ps_send[ch] = partial(other_base, ch)
        for copy in mate_copies(ch):
            copy.start()
    loads[2].wait()
    for ch in range(chunks):
        own[ch], own_sq[ch] = partial(own_base, ch)
    for ch in range(chunks):
        for copy in mate_copies(ch):
            copy.wait_recv()
        y_send[ch] = (own[ch] + p_recv[ch]).astype(BF16)
        ys_send[ch] = own_sq[ch] + ps_recv[ch]
        for r in range(1, peers):
            for copy in peer_copies(r, ch):
                copy.start()

    loads[3].wait()
    loads[4].wait()
    loads[5].wait()

    @pl.when(seq > 0)
    def _():
        edge.wait_recv()

    def gates(g, _):
        lanes = pl.ds(pl.multiple_of(g * BLK, BLK), BLK)
        soft = jnp.log1p(jnp.exp(-dparam[:, lanes]))
        row8 = lax.broadcasted_iota(jnp.int32, (1, 8, BLK), 1)

        def tile(t, _):
            x = ext[pl.ds(pl.multiple_of(t * CHUNK, CHUNK), CHUNK + HALO), lanes].astype(F32)
            total = shift[:, lanes] + taps[pl.ds(0, 1), lanes] * x[HALO:]
            for k in range(1, CONV):
                total = total + taps[pl.ds(k, 1), lanes] * pltpu.roll(x, k, 0)[HALO:]
            mixed = total.astype(BF16)
            inflow = jax.nn.sigmoid(jnp.dot(mixed, iw[g], preferred_element_type=F32) + ibias[:, lanes])
            rec = jax.nn.sigmoid(jnp.dot(mixed, dw[g], preferred_element_type=F32) + dbias[:, lanes])
            log_decay = (-decay_power * soft) * rec
            a = jnp.exp(log_decay)
            b = jnp.sqrt(neg_expm1(2.0 * log_decay)) * inflow * mixed.astype(F32)
            a = a.reshape(CHUNK // 8, 8, BLK)
            b = b.reshape(CHUNK // 8, 8, BLK)
            for k in (1, 2, 4):
                keep = row8 >= k
                b = b + a * jnp.where(keep, pltpu.roll(b, k, 1), 0.0)
                a = a * jnp.where(keep, pltpu.roll(a, k, 1), 1.0)
            here = pl.ds(pl.multiple_of(t * CHUNK, CHUNK), CHUNK)
            a_s[here, lanes] = a.reshape(CHUNK, BLK)
            b_s[here, lanes] = b.reshape(CHUNK, BLK)
            return 0

        lax.fori_loop(0, T // CHUNK, tile, 0)
        return 0

    lax.fori_loop(0, groups // 2, gates, 0)

    def z_copy(d, ch):
        at = rows(own_base, ch)
        return remote(kv.at[far - d, at], kv.at[far - d - 2, at], zs.at[d, ch], zr.at[d + 2, ch], (seq + 2, m))

    def z_arrival(d, ch):
        at = rows(own_base, ch)
        return remote(kv.at[far - d, at], kv.at[far - d, at], zs.at[d, ch], zr.at[d, ch], (seq, mate))

    def x_copy(d, e, ch):
        at = rows(own_base, ch)
        return remote(
            kv.at[far - d, at], kv.at[far - e, at], xs.at[d, ch], xr.at[e, ch], (seq + (e - d), m)
        )

    def x_arrival(d, ch):
        at = rows(own_base, ch)
        return remote(kv.at[far - d, at], kv.at[far - d, at], xs.at[d, ch], xr.at[d, ch], (seq, mate))

    def d_copy(d, ch):
        at = rows(own_base, ch)
        return remote(kv.at[far - d, at], kv.at[far - d, at], ds.at[d, ch], dr.at[d, ch], (seq, mate))

    def d_arrival(d, ch):
        at = rows(other_base, ch)
        return remote(kv.at[far - d, at], kv.at[far - d, at], ds.at[d, ch], dr.at[d, ch], (seq, mate))

    def even_copies(d, ch, act):
        if d + 2 <= far:
            @pl.when((seq >= d) & (seq + 2 < n))
            def _():
                act(z_copy(d, ch))
        if d >= 2:
            @pl.when((seq >= d) & (odd == 1))
            def _():
                act(x_copy(d, d - 1, ch))
        if d + 1 <= back:
            @pl.when((seq >= d) & (odd == 0))
            def _():
                act(x_copy(d, d + 1, ch))

    def mate_out(d, ch, act):
        if d <= back:
            @pl.when(seq >= d)
            def _():
                act(d_copy(d, ch))

    start = lambda copy: copy.start()
    features = C * mp
    for ch in range(chunks):
        for r in range(1, peers):
            for copy in peer_copies(r, ch):
                copy.wait_recv()
        total = y_send[ch].astype(F32)
        square = ys_send[ch]
        for r in range(1, peers):
            total = total + y_recv[r - 1, ch].astype(F32)
            square = square + ys_recv[r - 1, ch]
        inverse = 1.0 / jnp.sqrt(square / features + norm_epsilon)
        inverse = jnp.transpose(jnp.broadcast_to(inverse[:1], (128, CHUNK)))
        kv[far, rows(own_base, ch), :] = (total * inverse[:, :1]).astype(BF16)
        even_copies(0, ch, start)
        mate_out(0, ch, start)

    lax.fori_loop(groups // 2, groups, gates, 0)

    def forward(d):
        for ch in range(chunks):
            @pl.when(seq >= d)
            def _():
                z_arrival(d, ch).wait_recv()
            even_copies(d, ch, start)
            mate_out(d, ch, start)

    if far >= 2:
        forward(2)

    def carry_rows(j, state):
        factor, value = state
        at = pl.ds(pl.multiple_of(j * 8, 8), 8)
        a = a_s[at, :]
        b = b_s[at, :] + a * value
        a = a * factor
        a_s[at, :] = a
        b_s[at, :] = b
        return jnp.broadcast_to(a[7:8], (8, C)), jnp.broadcast_to(b[7:8], (8, C))

    factor, value = lax.fori_loop(0, T // 8, carry_rows, (jnp.ones((8, C), F32), jnp.zeros((8, C), F32)), unroll=4)
    pairs[seq, pl.ds(0, 1), :] = factor[:1]
    pairs[seq, pl.ds(1, 1), :] = value[:1]

    def pair_copy(j):
        return remote(pairs.at[seq], pairs.at[seq], csend.at[j], crecv.at[seq], (j, m))

    def pair_arrival(j):
        return remote(pairs.at[j], pairs.at[j], csend.at[j], crecv.at[j], (seq, mate))

    def send_pair(j, _):
        pair_copy(j).start()
        return 0

    lax.fori_loop(seq + 1, n, send_pair, 0)

    loads[7].wait()

    def scale_rows(j, _):
        at = pl.ds(pl.multiple_of(j * 64, 64), 64)
        q_v[at, :] = (q_v[at, :].astype(F32) * HD ** (-0.5)).astype(BF16)
        return 0

    lax.fori_loop(0, T // 64, scale_rows, 0)
    row = lax.broadcasted_iota(jnp.int32, (QROWS, QROWS), 0)
    col = lax.broadcasted_iota(jnp.int32, (QROWS, QROWS), 1)
    tiles = T // QROWS
    heads = q_v.shape[1] // HD

    def attend_tile(d, h, i):
        unit = h * tiles + i
        low, high = 0, T
        if d == 0:
            high = (i + 1) * QROWS
        if d == back:
            low = i * QROWS
        q = q_v[pl.ds(i * QROWS, QROWS), pl.ds(pl.multiple_of(h * HD, HD), HD)]
        keys = kv[far - d, pl.ds(low, high - low), pl.ds(0, HD)]
        values = kv[far - d, pl.ds(low, high - low), pl.ds(HD, HD)]
        s = lax.dot_general(q, keys, (((1,), (1,)), ((), ())), preferred_element_type=F32)
        parts = [s[:, k : k + QROWS] for k in range(0, high - low, QROWS)]
        if d == 0:
            parts[-1] = jnp.where(col <= row, parts[-1], masked_score)
        if d == back:
            parts[0] = jnp.where(col > row, parts[0], masked_score)
        peak = functools.reduce(jnp.maximum, parts)
        peak = jnp.max(peak, axis=1, keepdims=True)
        if d > 0:
            before = peak_s[unit][:, :1]
            peak = jnp.maximum(before, peak)
            alpha = jnp.exp(before - peak)
        parts = [jnp.exp(part - peak) for part in parts]
        summed = sum(part[:, k : k + 128] for part in parts for k in range(0, QROWS, 128))
        p = jnp.concatenate([part.astype(BF16) for part in parts], axis=1)
        gathered = jnp.dot(p, values, preferred_element_type=F32)
        if d > 0:
            summed = summed + alpha * sum_s[unit]
            gathered = gathered + alpha * acc_s[unit]
        peak_s[unit] = jnp.broadcast_to(peak, (QROWS, 128))
        sum_s[unit] = summed
        acc_s[unit] = gathered

    def attend(d):
        if d > back:
            return

        @pl.when(seq >= d)
        def _():
            for ch in range(chunks):
                d_arrival(d, ch).wait_recv()

            def head(h, _):
                for i in range(tiles):
                    attend_tile(d, h, i)
                return 0

            lax.fori_loop(0, heads, head, 0)

    def crossed(d):
        for ch in range(chunks):
            @pl.when(seq >= d)
            def _():
                x_arrival(d, ch).wait_recv()
            mate_out(d, ch, start)

    def join(j, incoming):
        pair_arrival(j).wait_recv()
        return pairs[j, pl.ds(0, 1), :] * incoming + pairs[j, pl.ds(1, 1), :]

    def finish_recurrence():
        incoming = lax.fori_loop(0, seq, join, jnp.zeros((1, C), F32))

        def finish(j, _):
            at = pl.ds(pl.multiple_of(j * 16, 16), 16)
            states = b_s[at, :] + a_s[at, :] * incoming
            v = gate[at, :].astype(F32)
            gelu = 0.5 * v * (1.0 + jnp.tanh(0.7978845608028654 * (v + 0.044715 * v * v * v)))
            rec_out[at, :] = (states * gelu).astype(BF16)
            return 0

        lax.fori_loop(0, T // 16, finish, 0)

    attend(0)
    for d in range(2, far + 1, 2):
        crossed(d - 1)
        if d == 2:
            loads[6].wait()
            finish_recurrence()
        attend(d)
        if d + 2 <= far:
            forward(d + 2)
        attend(d - 1)

    def settle(h, _):
        for i in range(tiles):
            unit = h * tiles + i
            scale = 1.0 / jnp.sum(sum_s[unit], axis=1, keepdims=True)
            at = (pl.ds(i * QROWS, QROWS), pl.ds(pl.multiple_of(h * HD, HD), HD))
            att_out[at] = (acc_s[unit] * scale).astype(BF16)
        return 0

    lax.fori_loop(0, heads, settle, 0)

    sent = lambda copy: copy.wait_send()
    for ch in range(chunks):
        for copy in mate_copies(ch):
            copy.wait_send()
        for r in range(1, peers):
            for copy in peer_copies(r, ch):
                copy.wait_send()
        for d in range(0, far + 1, 2):
            even_copies(d, ch, sent)
        for d in range(back + 1):
            mate_out(d, ch, sent)

    @pl.when(seq + 1 < n)
    def _():
        edge.wait_send()

    def pair_sent(j, _):
        pair_copy(j).wait_send()
        return 0

    lax.fori_loop(seq + 1, n, pair_sent, 0)


def shards(
    n, mp,
    branch_in, branch_gate, conv_taps, conv_shift, inflow_weight, inflow_bias, decay_weight, decay_bias,
    decay_param, stream, norm_gain, memory_weight, queries,
):
    T, C = branch_in.shape
    width = memory_weight.shape[1]
    back = WINDOW // T
    far = back + back % 2
    chunks = T // 2 // CHUNK
    groups = inflow_weight.shape[0]
    peers = mp // 2
    vmem = pl.BlockSpec(memory_space=pltpu.VMEM)
    hbm = pl.BlockSpec(memory_space=pl.ANY)
    dma = pltpu.SemaphoreType.DMA
    flat = lambda v: v.reshape(1, -1)
    others = max(peers - 1, 1)
    heads = queries.shape[1] // HD
    units = heads * (T // QROWS)
    return pl.pallas_call(
        functools.partial(exchange_kernel, n, mp, back, far),
        out_shape=(
            jax.ShapeDtypeStruct((T, C), BF16),
            jax.ShapeDtypeStruct(queries.shape, BF16),
        ),
        in_specs=[vmem] * 6 + [hbm] * 7,
        out_specs=(vmem, vmem),
        scratch_shapes=[
            pltpu.VMEM((far + 1, T, width), BF16),
            pltpu.VMEM(queries.shape, BF16),
            pltpu.VMEM((units, QROWS, HD), F32),
            pltpu.VMEM((units, QROWS, 128), F32),
            pltpu.VMEM((units, QROWS, 128), F32),
            pltpu.VMEM((T + HALO, C), BF16),
            pltpu.VMEM((T, C), BF16),
            pltpu.VMEM((groups, BLK, BLK), BF16),
            pltpu.VMEM((groups, BLK, BLK), BF16),
            pltpu.VMEM((T, C), BF16),
            pltpu.VMEM((C, width), BF16),
            pltpu.VMEM((T, C), F32),
            pltpu.VMEM((T, C), F32),
            pltpu.VMEM((n, 2, C), F32),
            pltpu.VMEM((chunks, CHUNK, width), F32),
            pltpu.VMEM((chunks, CHUNK, width), F32),
            pltpu.VMEM((chunks, CHUNK, width), F32),
            pltpu.VMEM((chunks, 8, CHUNK), F32),
            pltpu.VMEM((chunks, 8, CHUNK), F32),
            pltpu.VMEM((chunks, 8, CHUNK), F32),
            pltpu.VMEM((chunks, CHUNK, width), BF16),
            pltpu.VMEM((others, chunks, CHUNK, width), BF16),
            pltpu.VMEM((chunks, 8, CHUNK), F32),
            pltpu.VMEM((others, chunks, 8, CHUNK), F32),
            dma((8,)),
            dma((2,)),
            dma((4, chunks)),
            dma((4, others, chunks)),
            dma((n,)),
            dma((n,)),
        ]
        + [dma((far + 3, chunks))] * 6,
        compiler_params=pltpu.CompilerParams(collective_id=0, has_side_effects=True),
    )(
        conv_taps, flat(conv_shift), flat(inflow_bias), flat(decay_bias), flat(decay_param), flat(norm_gain),
        branch_in, branch_gate, inflow_weight, decay_weight, stream, memory_weight, queries,
    )


def solution(mesh):
    return jax.shard_map(
        functools.partial(shards, mesh.shape["seq"], mesh.shape["mp"]),
        mesh=mesh,
        in_specs=(
            P("seq", "mp"),
            P("seq", "mp"),
            P(None, "mp"),
            P("mp"),
            P("mp", None, None),
            P("mp"),
            P("mp", None, None),
            P("mp"),
            P("mp"),
            P("seq", "mp"),
            P("mp"),
            P("mp", None),
            P("seq", "mp"),
        ),
        out_specs=(P("seq", "mp"), P("seq", "mp")),
        check_vma=False,
    )
```
